32 devices in a mesh: tm: 8 (over z, y), series: 4 (over x, core).
Axes of the slice: x: 2, y: 2, z: 4, core: 2. Of those that a mesh axis runs over, the one named last changes fastest.
Arguments:
- signal: float32 [64, 262144], P('series', 'tm')
- valid_start: int32 [64], replicated, may hold values from 0 to 65535
- valid_end: int32 [64], replicated, may hold values from 196609 to 262144
Outputs:
- smooth: float32 [64, 262144], P('series', 'tm')
- slope: float32 [64, 262144], P('series', 'tm')
- covariance: float32 [64, 64], P('series')
The draws below stay inside these ranges and needn't reach their ends.
Inputs may be any that keep to these rules, and one draw needn't show every extreme that they name: `valid_end`: end of the valid samples of each series.
All inputs are finite; a program needn't handle non-finite values.
Results may differ from the reference program's by a relative error of at most 0.00015.
Values sent between devices are 32-bit elements; how exact they have to be, the bound alone decides.
A program may use at most 64 MiB of HBM per device.

```python
import math
import jax
import jax.numpy as jnp
from jax import lax

HALF = 16
S = 64
NT = 262144


def draw_signal(key, part):
    keys = jax.random.split(jax.random.fold_in(key, 17), 6)
    times = jnp.arange(NT).astype(jnp.float32) / NT
    rising = 0.5 + times
    mixing = jax.random.uniform(keys[0], (S, 1), jnp.float32, -1.0, 1.0)
    phase = jax.random.uniform(keys[4], (S, 1), jnp.float32, 0.0, 2.0 * math.pi)
    freq = jax.random.uniform(keys[5], (S, 1), jnp.float32, 3.0, 9.0)
    trend = jnp.sin(2.0 * math.pi * freq * times[None, :] + phase)
    common = jax.random.normal(keys[1], (NT,), jnp.float32)
    own = jax.random.normal(keys[2], (S, NT), jnp.float32)
    noise = 0.8 * rising[None, :] * (mixing * common[None, :] + own)
    return trend + noise


def set_ends(array, key, smallest, largest):
    dims = array.shape
    place = [jax.random.randint(jax.random.fold_in(key, axis), (), 0, dims[axis]) for axis in range(len(dims))]
    array = array.at[tuple(place)].set(smallest)
    longest = dims.index(max(dims))
    place[longest] = (place[longest] + 1) % dims[longest]
    return array.at[tuple(place)].set(largest)


def setup_inputs(seed: int = 0) -> dict:
    seeds = jax.random.split(jax.random.key(seed), 4)
    return {
        "signal": draw_signal(jax.random.fold_in(seeds[3], 71), 0),
        "valid_start": set_ends(jax.random.randint(seeds[1], (S,), 0, NT // 4), jax.random.fold_in(seeds[1], 1), 0, (NT // 4) - 1).astype(jnp.int32),
        "valid_end": set_ends(jax.random.randint(seeds[2], (S,), NT - NT // 4 + 1, NT + 1), jax.random.fold_in(seeds[2], 1), NT - NT // 4 + 1, NT).astype(jnp.int32),
    }


def reference(signal, valid_start, valid_end):
    taps = 2 * HALF + 1
    offsets = jnp.arange(-HALF, HALF + 1).astype(jnp.float32)
    second = jnp.sum(offsets * offsets)
    centre_sq = second / taps
    curved = offsets * offsets - centre_sq
    fourth = jnp.sum(curved * curved)
    padded = jnp.pad(signal, ((0, 0), (HALF, HALF)))
    level = jnp.zeros_like(signal)
    tilt = jnp.zeros_like(signal)
    bend = jnp.zeros_like(signal)
    for m in range(taps):
        window = padded[:, m:m + NT]
        level = level + window * (1.0 / taps)
        tilt = tilt + window * (offsets[m] / second)
        bend = bend + window * (curved[m] / fourth)
    first = valid_start.astype(jnp.int32)[:, None]
    last = valid_end.astype(jnp.int32)[:, None]
    moment = jnp.arange(NT, dtype=jnp.int32)[None, :]
    centre = jnp.clip(moment, first + HALF, last - HALF - 1).astype(jnp.int32)
    along = (moment - centre).astype(jnp.float32)
    lv = jnp.take_along_axis(level, centre, axis=1)
    tl = jnp.take_along_axis(tilt, centre, axis=1)
    bd = jnp.take_along_axis(bend, centre, axis=1)
    inside = (moment >= first) & (moment < last)
    smooth = jnp.where(inside, lv + tl * along + bd * (along * along - centre_sq), 0.0)
    slope = jnp.where(inside, HALF * (tl + 2.0 * along * bd), 0.0)
    resid = jnp.where(inside, signal - smooth, 0.0)
    gram = lax.dot_general(resid, resid, (((1,), (1,)), ((), ())), precision=lax.Precision.HIGHEST, preferred_element_type=jnp.float32)
    correlation = (jnp.minimum(last, valid_end[None, :]) - jnp.maximum(first, valid_start[None, :])).astype(jnp.float32)
    return smooth, slope, gram / correlation
```

```python
import functools

import jax
import jax.numpy as jnp
from jax import lax
from jax.experimental import pallas as pl
from jax.experimental.pallas import tpu as pltpu
from jax.sharding import PartitionSpec as P

HALF = 16
LANE = 128
TAPS = 2 * HALF + 1
SECOND = float(sum(j * j for j in range(-HALF, HALF + 1)))
CENTRE_SQ = SECOND / TAPS
FOURTH = float(sum((j * j - CENTRE_SQ) ** 2 for j in range(-HALF, HALF + 1)))
MESH = pl.DeviceIdType.MESH


def chunk_of(quarter):
    chunk = 2048
    while quarter % chunk:
        chunk //= 2
    return chunk


def kernel(
    n_s, n_t, rows, width, chunk,
    vs_hbm, ve_hbm, sig_hbm,
    smooth, slope, cov,
    vs, ve, ext, wts, wins, coef, ends, res, mixed, halo, part, r1, mine, r2,
    load_sem, bound_sem, halo_send, halo_recv, send_sem, recv_sem, s1_send, s1_recv, s2_send, s2_recv,
):
    s = lax.axis_index("series")
    t = lax.axis_index("tm")
    quarter = width // n_s
    per = quarter // chunk
    steps = n_s * per
    sends = (n_s - 1) * per
    total = n_s * rows
    f32 = jnp.float32

    load = pltpu.make_async_copy(sig_hbm, ext.at[:, pl.ds(LANE, width)], load_sem)
    load.start()
    starts = pltpu.make_async_copy(vs_hbm, vs, bound_sem.at[0])
    stops = pltpu.make_async_copy(ve_hbm, ve, bound_sem.at[1])
    starts.start()
    stops.start()
    barrier = pltpu.get_barrier_semaphore()
    for d in range(1, n_s):
        pl.semaphore_signal(barrier, inc=1, device_id={"series": lax.rem(s + d, n_s)}, device_id_type=MESH)
    for d in range(1, n_t):
        pl.semaphore_signal(barrier, inc=1, device_id={"tm": lax.rem(t + d, n_t)}, device_id_type=MESH)

    tap = lax.broadcasted_iota(jnp.int32, (2 * LANE, LANE), 0) - lax.broadcasted_iota(jnp.int32, (2 * LANE, LANE), 1) - HALF
    near = (tap >= -HALF) & (tap <= HALF)
    tap = tap.astype(f32)
    wts[:, :LANE] = jnp.where(near, 1.0 / TAPS - (tap * tap - CENTRE_SQ) * (CENTRE_SQ / FOURTH), 0.0)
    wts[:, LANE:] = jnp.where(near, tap * (HALF / SECOND), 0.0)
    ext[:, :LANE] = jnp.zeros((rows, LANE), f32)
    ext[:, LANE + width :] = jnp.zeros((rows, LANE), f32)

    starts.wait()
    stops.wait()
    row = lax.broadcasted_iota(jnp.int32, (rows, LANE), 0)
    begin = t * width
    first = jnp.zeros((rows, LANE), jnp.int32)
    last = jnp.zeros((rows, LANE), jnp.int32)
    for i in range(rows):
        first = jnp.where(row == i, vs[s * rows + i], first)
        last = jnp.where(row == i, ve[s * rows + i], last)
    ends[0] = first - begin
    ends[1] = last - begin

    def spots():
        low = ends[0] + LANE
        high = ends[1] - TAPS + LANE
        return low, high

    def tile_of(spot):
        return lax.shift_right_arithmetic(spot, LANE.bit_length() - 1)

    def collect(n, tile, wins):
        low, high = spots()
        wins = list(wins)
        for side, spot in ((0, low), (1, high)):
            wins[2 * side] = jnp.where(tile_of(spot) == n, tile, wins[2 * side])
            wins[2 * side + 1] = jnp.where(tile_of(spot) == n - 1, tile, wins[2 * side + 1])
        return tuple(wins)

    def held(wins):
        lanes = lax.broadcasted_iota(jnp.int32, (rows, LANE), 1)
        for side, spot in enumerate(spots()):
            off = spot - tile_of(spot) * LANE + HALF
            near, far = lanes - off, lanes + LANE - off
            sums = []
            for j, win in ((near, wins[2 * side]), (far, wins[2 * side + 1])):
                win = jnp.where((j >= -HALF) & (j <= HALF), win, 0.0)
                j = j.astype(f32)
                sums.append((win, win * j, win * (j * j - CENTRE_SQ)))
            for m, scale in enumerate((1.0 / TAPS, 1.0 / SECOND, 1.0 / FOURTH)):
                value = jnp.sum(sums[0][m] + sums[1][m], axis=1, keepdims=True) * scale
                coef[3 * side + m] = jnp.broadcast_to(value, (rows, LANE))

    load.wait()

    group = 8
    while (width // LANE) % group:
        group //= 2

    def gather(g, found):
        for n in range(group):
            at = g * group + n
            found = collect(at + 1, ext[:, pl.ds(pl.multiple_of((at + 1) * LANE, LANE), LANE)], found)
        return found

    found = lax.fori_loop(0, width // LANE // group, gather, (jnp.zeros((rows, LANE), f32),) * 4)
    for w in range(4):
        wins[w] = found[w]
    held(found)
    pl.semaphore_wait(barrier, n_s - 1 + n_t - 1)

    right, left = lax.rem(t + 1, n_t), lax.rem(t + n_t - 1, n_t)
    to_right = pltpu.make_async_remote_copy(
        ext.at[:, pl.ds(width, LANE)], halo.at[0], halo_send.at[0], halo_recv.at[0],
        device_id={"tm": right}, device_id_type=MESH)
    to_left = pltpu.make_async_remote_copy(
        ext.at[:, pl.ds(LANE, LANE)], halo.at[1], halo_send.at[1], halo_recv.at[1],
        device_id={"tm": left}, device_id_type=MESH)
    to_right.start()
    to_left.start()

    def offset(qi):
        if n_s == 4:
            odd = lax.rem(s, 2)
            return jnp.where(qi == 0, 2, jnp.where(qi == 1, 3 - 2 * odd, jnp.where(qi == 2, 1 + 2 * odd, 0)))
        return lax.rem(qi + 1, n_s)

    def place(k):
        qi = k // per
        q = lax.rem(s + offset(qi), n_s)
        j = lax.rem(lax.rem(k, per) + jnp.where(q == 0, 1, 0), per)
        return q, j

    def transfer(k):
        q, j = place(k)
        return pltpu.make_async_remote_copy(
            res.at[:, pl.ds(pl.multiple_of(q * quarter + j * chunk, chunk), chunk)],
            mixed.at[s, :, pl.ds(pl.multiple_of(j * chunk, chunk), chunk)],
            send_sem.at[k], recv_sem.at[k],
            device_id={"series": q}, device_id_type=MESH)

    tiles = chunk // LANE

    def spread(v):
        return jnp.concatenate([v] * tiles, axis=1)

    def step(k, carry):
        @pl.when(k == per - 1)
        def _():
            to_right.wait_recv()
            to_left.wait_recv()
            before = jnp.where(t == 0, 0.0, halo[0])
            after = jnp.where(t == n_t - 1, 0.0, halo[1])
            ext[:, :LANE] = before
            ext[:, LANE + width :] = after
            final = tuple(wins[w] for w in range(4))
            final = collect(0, before, final)
            held(collect(width // LANE + 1, after, final))

        q, j = place(k)
        base = pl.multiple_of(q * quarter + j * chunk, chunk)
        v = ext[:, pl.ds(base, chunk + 2 * LANE)]
        moved = pltpu.roll(v, chunk + LANE + HALF, 1)
        lines = jnp.concatenate([moved[:, n * LANE : (n + 2) * LANE] for n in range(tiles)], axis=0)
        out = jnp.dot(lines, wts[...], precision=lax.Precision.HIGHEST, preferred_element_type=f32)
        sm = jnp.concatenate([out[n * rows : (n + 1) * rows, :LANE] for n in range(tiles)], axis=1)
        sl = jnp.concatenate([out[n * rows : (n + 1) * rows, LANE:] for n in range(tiles)], axis=1)
        moment = base + lax.broadcasted_iota(jnp.int32, (rows, chunk), 1)
        low = moment - spread(ends[0])
        high = moment - spread(ends[1])
        inside = (low >= 0) & (high < 0)
        below = low < HALF
        above = high >= -HALF
        along = jnp.where(below, low - HALF, high + HALF + 1).astype(f32)
        lv = jnp.where(below, spread(coef[0]), spread(coef[3]))
        tl = jnp.where(below, spread(coef[1]), spread(coef[4]))
        bd = jnp.where(below, spread(coef[2]), spread(coef[5]))
        end = below | above
        sm = jnp.where(end, lv + tl * along + bd * (along * along - CENTRE_SQ), sm)
        sl = jnp.where(end, HALF * (tl + 2.0 * along * bd), sl)
        sm = jnp.where(inside, sm, 0.0)
        smooth[:, pl.ds(base, chunk)] = sm
        slope[:, pl.ds(base, chunk)] = jnp.where(inside, sl, 0.0)
        rs = jnp.where(inside, v[:, LANE : LANE + chunk] - sm, 0.0)

        @pl.when(k < sends)
        def _():
            res[:, pl.ds(base, chunk)] = rs

        @pl.when(k >= sends)
        def _():
            mixed[s, :, pl.ds(pl.multiple_of(j * chunk, chunk), chunk)] = rs

        @pl.when((k >= 1) & (k <= sends))
        def _():
            transfer(k - 1).start()

        return carry

    lax.fori_loop(0, steps, step, 0)

    def arrival(k, i):
        src = lax.rem(s + n_s - offset(k // per), n_s)
        j = lax.rem(i + jnp.where(s == 0, 1, 0), per)
        return pltpu.make_async_remote_copy(
            res.at[:, pl.ds(0, chunk)],
            mixed.at[src, :, pl.ds(pl.multiple_of(j * chunk, chunk), chunk)],
            send_sem.at[k], recv_sem.at[k],
            device_id={"series": src}, device_id_type=MESH)

    gram = jnp.zeros((2 * total, 2 * total), f32)
    for i in range(per):
        for qi in range(n_s - 1):
            arrival(qi * per + i, i).wait_recv()
        j = lax.rem(i + jnp.where(s == 0, 1, 0), per)
        x = jnp.concatenate(
            [mixed[g, :, pl.ds(pl.multiple_of(j * chunk, chunk), chunk)] for g in range(n_s)], axis=0)
        hi = x.astype(jnp.bfloat16)
        lo = (x - hi.astype(f32)).astype(jnp.bfloat16)
        z = jnp.concatenate([hi, lo], axis=0)
        gram = gram + lax.dot_general(z, z, (((1,), (1,)), ((), ())), preferred_element_type=f32)
    both = gram[:total] + gram[total:]
    both = both + pltpu.roll(both, total, 1)
    for g in range(n_s):
        part[g] = both[g * rows : (g + 1) * rows]

    def first_stage(d):
        peer = lax.rem(s + d, n_s)
        return pltpu.make_async_remote_copy(
            part.at[peer], r1.at[d - 1], s1_send.at[d - 1], s1_recv.at[d - 1],
            device_id={"series": peer}, device_id_type=MESH)

    for d in range(1, n_s):
        first_stage(d).start()

    lane = lax.broadcasted_iota(jnp.int32, (rows, 2 * total), 1)
    first_k = jnp.zeros((rows, 2 * total), jnp.int32)
    last_k = jnp.zeros((rows, 2 * total), jnp.int32)
    for i in range(total):
        first_k = jnp.where(lane == i, vs[i], first_k)
        last_k = jnp.where(lane == i, ve[i], last_k)
    count = (jnp.minimum(last_k, last) - jnp.maximum(first_k, first)).astype(f32)

    own = part[s]
    for d in range(1, n_s):
        first_stage(d).wait_recv()
        own = own + r1[d - 1]
    mine[...] = own

    def second_stage(d):
        return pltpu.make_async_remote_copy(
            mine, r2.at[t], s2_send.at[d - 1], s2_recv.at[d - 1],
            device_id={"tm": lax.rem(t + d, n_t)}, device_id_type=MESH)

    def second_arrival(d):
        src = lax.rem(t + n_t - d, n_t)
        return pltpu.make_async_remote_copy(
            mine, r2.at[src], s2_send.at[d - 1], s2_recv.at[d - 1],
            device_id={"tm": src}, device_id_type=MESH)

    for d in range(1, n_t):
        second_stage(d).start()
    r2[t] = own
    for k in range(sends):
        transfer(k).wait_send()
    to_right.wait_send()
    to_left.wait_send()
    for d in range(1, n_s):
        first_stage(d).wait_send()
    for d in range(1, n_t):
        second_arrival(d).wait_recv()
    full = r2[0]
    for d in range(1, n_t):
        full = full + r2[d]
    cov[...] = (full / count)[:, :total]
    for d in range(1, n_t):
        second_stage(d).wait_send()


def solution(mesh):
    n_t, n_s = mesh.shape["tm"], mesh.shape["series"]

    def shards(signal, valid_start, valid_end):
        rows, width = signal.shape
        total = rows * n_s
        quarter = width // n_s
        chunk = chunk_of(quarter)
        sends = (n_s - 1) * (quarter // chunk)
        f32 = jnp.float32
        dma = pltpu.SemaphoreType.DMA
        return pl.pallas_call(
            functools.partial(kernel, n_s, n_t, rows, width, chunk),
            out_shape=(
                jax.ShapeDtypeStruct((rows, width), f32),
                jax.ShapeDtypeStruct((rows, width), f32),
                jax.ShapeDtypeStruct((rows, total), f32),
            ),
            in_specs=[
                pl.BlockSpec(memory_space=pltpu.HBM),
                pl.BlockSpec(memory_space=pltpu.HBM),
                pl.BlockSpec(memory_space=pltpu.HBM),
            ],
            out_specs=(pl.BlockSpec(memory_space=pltpu.VMEM),) * 3,
            scratch_shapes=[
                pltpu.SMEM((total,), jnp.int32),
                pltpu.SMEM((total,), jnp.int32),
                pltpu.VMEM((rows, width + 2 * LANE), f32),
                pltpu.VMEM((2 * LANE, 2 * LANE), f32),
                pltpu.VMEM((4, rows, LANE), f32),
                pltpu.VMEM((6, rows, LANE), f32),
                pltpu.VMEM((2, rows, LANE), jnp.int32),
                pltpu.VMEM((rows, width), f32),
                pltpu.VMEM((n_s, rows, quarter), f32),
                pltpu.VMEM((2, rows, LANE), f32),
                pltpu.VMEM((n_s, rows, 2 * total), f32),
                pltpu.VMEM((n_s - 1, rows, 2 * total), f32),
                pltpu.VMEM((rows, 2 * total), f32),
                pltpu.VMEM((n_t, rows, 2 * total), f32),
                dma,
                dma((2,)),
                dma((2,)),
                dma((2,)),
                dma((sends,)),
                dma((sends,)),
                dma((n_s - 1,)),
                dma((n_s - 1,)),
                dma((n_t - 1,)),
                dma((n_t - 1,)),
            ],
            compiler_params=pltpu.CompilerParams(
                collective_id=0, has_side_effects=True, vmem_limit_bytes=67043328 - 8 * rows * width - rows * width
            ),
        )(valid_start, valid_end, signal)

    in_specs = (P("series", "tm"), P(), P())
    out_specs = (P("series", "tm"), P("series", "tm"), P("series", None))
    return jax.shard_map(shards, mesh=mesh, in_specs=in_specs, out_specs=out_specs, check_vma=False)
```

```python
import functools

import jax
import jax.numpy as jnp
from jax import lax
from jax.experimental import pallas as pl
from jax.experimental.pallas import tpu as pltpu
from jax.sharding import PartitionSpec as P

HALF = 16
LANE = 128
TAPS = 2 * HALF + 1
SECOND = float(sum(j * j for j in range(-HALF, HALF + 1)))
CENTRE_SQ = SECOND / TAPS
FOURTH = float(sum((j * j - CENTRE_SQ) ** 2 for j in range(-HALF, HALF + 1)))
MESH = pl.DeviceIdType.MESH


def chunk_of(quarter):
    chunk = 1024
    while quarter % chunk:
        chunk //= 2
    return chunk


def kernel(
    n_s, n_t, rows, width, chunk,
    vs_hbm, ve_hbm, sig_hbm,
    smooth, slope, cov,
    vs, ve, ext, wts, ends, res, mixed, halo, part, r1, mine, r2,
    load_sem, bound_sem, halo_send, halo_recv, send_sem, recv_sem, s1_send, s1_recv, s2_send, s2_recv,
):
    s = lax.axis_index("series")
    t = lax.axis_index("tm")
    quarter = width // n_s
    per = quarter // chunk
    steps = n_s * per
    sends = (n_s - 1) * per
    total = n_s * rows
    tiles = chunk // LANE
    f32 = jnp.float32

    starts = pltpu.make_async_copy(vs_hbm, vs, bound_sem.at[0])
    stops = pltpu.make_async_copy(ve_hbm, ve, bound_sem.at[1])
    starts.start()
    stops.start()
    def offset(qi):
        if n_s == 4:
            odd = lax.rem(s, 2)
            return jnp.where(qi == 0, 2, jnp.where(qi == 1, 3 - 2 * odd, jnp.where(qi == 2, 1 + 2 * odd, 0)))
        return lax.rem(qi + 1, n_s)

    def load(qi):
        q = lax.rem(s + offset(qi), n_s)
        return pltpu.make_async_copy(
            sig_hbm.at[:, pl.ds(pl.multiple_of(q * quarter, LANE), quarter)],
            ext.at[:, pl.ds(pl.multiple_of(q * quarter + LANE, LANE), quarter)],
            load_sem.at[qi])

    for qi in range(n_s):
        load(qi).start()
    barrier = pltpu.get_barrier_semaphore()
    for d in range(1, n_s):
        pl.semaphore_signal(barrier, inc=1, device_id={"series": lax.rem(s + d, n_s)}, device_id_type=MESH)
    for d in range(1, n_t):
        pl.semaphore_signal(barrier, inc=1, device_id={"tm": lax.rem(t + d, n_t)}, device_id_type=MESH)

    tap = lax.broadcasted_iota(jnp.int32, (2 * LANE, LANE), 0) - lax.broadcasted_iota(jnp.int32, (2 * LANE, LANE), 1) - HALF
    near = (tap >= -HALF) & (tap <= HALF)
    tap = tap.astype(f32)
    wts[:, :LANE] = jnp.where(near, 1.0 / TAPS - (tap * tap - CENTRE_SQ) * (CENTRE_SQ / FOURTH), 0.0)
    wts[:, LANE:] = jnp.where(near, tap * (HALF / SECOND), 0.0)
    ext[:, :LANE] = jnp.zeros((rows, LANE), f32)
    ext[:, LANE + width :] = jnp.zeros((rows, LANE), f32)

    starts.wait()
    stops.wait()
    row = lax.broadcasted_iota(jnp.int32, (rows, LANE), 0)
    begin = t * width
    first = jnp.zeros((rows, LANE), jnp.int32)
    last = jnp.zeros((rows, LANE), jnp.int32)
    for i in range(rows):
        first = jnp.where(row == i, vs[s * rows + i], first)
        last = jnp.where(row == i, ve[s * rows + i], last)
    ends[0] = first - begin
    ends[1] = last - begin

    def held(v, base):
        lanes = lax.broadcasted_iota(jnp.int32, (rows, LANE), 1)
        found = []
        for spot in (ends[0] + LANE - base, ends[1] - TAPS + LANE - base):
            tile = lax.shift_right_arithmetic(spot, LANE.bit_length() - 1)
            pair = [jnp.zeros((rows, LANE), f32)] * 2
            for n in range(tiles + 1):
                here = tile == n
                for w in range(2):
                    pair[w] = jnp.where(here, v[:, (n + w) * LANE : (n + w + 1) * LANE], pair[w])
            j = lanes - (spot - tile * LANE + HALF)
            sums = []
            for j, win in ((j, pair[0]), (j + LANE, pair[1])):
                win = jnp.where((j >= -HALF) & (j <= HALF), win, 0.0)
                j = j.astype(f32)
                sums.append((win, win * j, win * (j * j - CENTRE_SQ)))
            for m, scale in enumerate((1.0 / TAPS, 1.0 / SECOND, 1.0 / FOURTH)):
                value = jnp.sum(sums[0][m] + sums[1][m], axis=1, keepdims=True) * scale
                found.append(jnp.broadcast_to(value, (rows, LANE)))
        return found

    right, left = lax.rem(t + 1, n_t), lax.rem(t + n_t - 1, n_t)
    to_right = pltpu.make_async_remote_copy(
        ext.at[:, pl.ds(width, LANE)], halo.at[0], halo_send.at[0], halo_recv.at[0],
        device_id={"tm": right}, device_id_type=MESH)
    to_left = pltpu.make_async_remote_copy(
        ext.at[:, pl.ds(LANE, LANE)], halo.at[1], halo_send.at[1], halo_recv.at[1],
        device_id={"tm": left}, device_id_type=MESH)
    def place(k):
        qi = k // per
        q = lax.rem(s + offset(qi), n_s)
        j = lax.rem(lax.rem(k, per) + 1, per)
        return q, j

    def transfer(k):
        q, j = place(k)
        return pltpu.make_async_remote_copy(
            res.at[:, pl.ds(pl.multiple_of(q * quarter + j * chunk, chunk), chunk)],
            mixed.at[s, :, pl.ds(pl.multiple_of(j * chunk, chunk), chunk)],
            send_sem.at[k], recv_sem.at[k],
            device_id={"series": q}, device_id_type=MESH)

    def spread(v):
        return jnp.concatenate([v] * tiles, axis=1)

    def step(k, carry):
        @pl.when(k == 0)
        def _():
            load(0).wait()

        @pl.when(k == 1)
        def _():
            for qi in range(1, n_s):
                load(qi).wait()

        @pl.when(k == per - 2)
        def _():
            to_right.wait_recv()
            to_left.wait_recv()
            ext[:, :LANE] = jnp.where(t == 0, 0.0, halo[0])
            ext[:, LANE + width :] = jnp.where(t == n_t - 1, 0.0, halo[1])

        q, j = place(k)
        base = pl.multiple_of(q * quarter + j * chunk, chunk)
        v = ext[:, pl.ds(base, chunk + 2 * LANE)]
        moved = pltpu.roll(v, chunk + LANE + HALF, 1)
        lines = jnp.concatenate([moved[:, n * LANE : (n + 2) * LANE] for n in range(tiles)], axis=0)
        out = jnp.dot(lines, wts[...], precision=lax.Precision.HIGHEST, preferred_element_type=f32)
        sm = jnp.concatenate([out[n * rows : (n + 1) * rows, :LANE] for n in range(tiles)], axis=1)
        sl = jnp.concatenate([out[n * rows : (n + 1) * rows, LANE:] for n in range(tiles)], axis=1)
        moment = base + lax.broadcasted_iota(jnp.int32, (rows, chunk), 1)
        low = moment - spread(ends[0])
        high = moment - spread(ends[1])
        coef = held(v, base)
        inside = (low >= 0) & (high < 0)
        below = low < HALF
        above = high >= -HALF
        along = jnp.where(below, low - HALF, high + HALF + 1).astype(f32)
        lv = jnp.where(below, spread(coef[0]), spread(coef[3]))
        tl = jnp.where(below, spread(coef[1]), spread(coef[4]))
        bd = jnp.where(below, spread(coef[2]), spread(coef[5]))
        end = below | above
        sm = jnp.where(end, lv + tl * along + bd * (along * along - CENTRE_SQ), sm)
        sl = jnp.where(end, HALF * (tl + 2.0 * along * bd), sl)
        sm = jnp.where(inside, sm, 0.0)
        smooth[:, pl.ds(base, chunk)] = sm
        slope[:, pl.ds(base, chunk)] = jnp.where(inside, sl, 0.0)
        rs = jnp.where(inside, v[:, LANE : LANE + chunk] - sm, 0.0)

        @pl.when(k < sends)
        def _():
            res[:, pl.ds(base, chunk)] = rs

        @pl.when(k >= sends)
        def _():
            mixed[s, :, pl.ds(pl.multiple_of(j * chunk, chunk), chunk)] = rs

        @pl.when(k == 0)
        def _():
            pl.semaphore_wait(barrier, n_s - 1 + n_t - 1)

        @pl.when(k == 1)
        def _():
            to_right.start()
            to_left.start()

        @pl.when((k >= 1) & (k <= sends))
        def _():
            transfer(k - 1).start()

        return carry

    lax.fori_loop(0, steps, step, 0)

    def arrival(k, i):
        src = lax.rem(s + n_s - offset(k // per), n_s)
        j = (i + 1) % per
        return pltpu.make_async_remote_copy(
            res.at[:, pl.ds(0, chunk)],
            mixed.at[src, :, pl.ds(pl.multiple_of(j * chunk, chunk), chunk)],
            send_sem.at[k], recv_sem.at[k],
            device_id={"series": src}, device_id_type=MESH)

    half = rows // 2
    left_half = lax.broadcasted_iota(jnp.int32, (half, 2 * total), 1) < total

    def pack(v):
        return jnp.where(left_half, v[:half], v[half:])

    gram = jnp.zeros((2 * total, 2 * total), f32)
    for i in range(per):
        for qi in range(n_s - 1):
            arrival(qi * per + i, i).wait_recv()
        j = (i + 1) % per
        x = jnp.concatenate(
            [mixed[g, :, pl.ds(pl.multiple_of(j * chunk, chunk), chunk)] for g in range(n_s)], axis=0)
        hi = x.astype(jnp.bfloat16)
        lo = (x - hi.astype(f32)).astype(jnp.bfloat16)
        z = jnp.concatenate([hi, lo], axis=0)
        gram = gram + lax.dot_general(z, z, (((1,), (1,)), ((), ())), preferred_element_type=f32)
    both = gram[:total] + gram[total:]
    both = both + pltpu.roll(both, total, 1)
    for g in range(n_s):
        part[g] = pack(both[g * rows : (g + 1) * rows])

    def first_stage(d):
        peer = lax.rem(s + d, n_s)
        return pltpu.make_async_remote_copy(
            part.at[peer], r1.at[d - 1], s1_send.at[d - 1], s1_recv.at[d - 1],
            device_id={"series": peer}, device_id_type=MESH)

    for d in range(1, n_s):
        first_stage(d).start()

    lane = lax.broadcasted_iota(jnp.int32, (rows, 2 * total), 1)
    lane = jnp.where(lane < total, lane, lane - total)
    first_k = jnp.zeros((rows, 2 * total), jnp.int32)
    last_k = jnp.zeros((rows, 2 * total), jnp.int32)
    for i in range(total):
        first_k = jnp.where(lane == i, vs[i], first_k)
        last_k = jnp.where(lane == i, ve[i], last_k)
    count = pack((jnp.minimum(last_k, last) - jnp.maximum(first_k, first)).astype(f32))

    own = part[s]
    for d in range(1, n_s):
        first_stage(d).wait_recv()
        own = own + r1[d - 1]
    mine[...] = own

    def second_stage(d):
        return pltpu.make_async_remote_copy(
            mine, r2.at[t], s2_send.at[d - 1], s2_recv.at[d - 1],
            device_id={"tm": lax.rem(t + d, n_t)}, device_id_type=MESH)

    def second_arrival(d):
        src = lax.rem(t + n_t - d, n_t)
        return pltpu.make_async_remote_copy(
            mine, r2.at[src], s2_send.at[d - 1], s2_recv.at[d - 1],
            device_id={"tm": src}, device_id_type=MESH)

    for d in range(1, n_t):
        second_stage(d).start()
    r2[t] = own
    for k in range(sends):
        transfer(k).wait_send()
    to_right.wait_send()
    to_left.wait_send()
    for d in range(1, n_s):
        first_stage(d).wait_send()
    for d in range(1, n_t):
        second_arrival(d).wait_recv()
    full = r2[0]
    for d in range(1, n_t):
        full = full + r2[d]
    full = full / count
    cov[:half] = full[:, :total]
    cov[half:] = pltpu.roll(full, total, 1)[:, :total]
    for d in range(1, n_t):
        second_stage(d).wait_send()


FLUSHES = 4


def flush(smooth, slope, cov, smooth_out, slope_out, cov_out, sems, cov_sem):
    piece = smooth.shape[1] // FLUSHES
    copies = [pltpu.make_async_copy(cov, cov_out, cov_sem)]
    for i in range(FLUSHES):
        span = pl.ds(i * piece, piece)
        copies.append(pltpu.make_async_copy(smooth.at[:, span], smooth_out.at[:, span], sems.at[2 * i]))
        copies.append(pltpu.make_async_copy(slope.at[:, span], slope_out.at[:, span], sems.at[2 * i + 1]))
    for copy in copies:
        copy.start()
    for copy in copies:
        copy.wait()


def solution(mesh):
    n_t, n_s = mesh.shape["tm"], mesh.shape["series"]

    def shards(signal, valid_start, valid_end):
        rows, width = signal.shape
        total = rows * n_s
        quarter = width // n_s
        chunk = chunk_of(quarter)
        sends = (n_s - 1) * (quarter // chunk)
        f32 = jnp.float32
        dma = pltpu.SemaphoreType.DMA
        kept = pl.pallas_call(
            functools.partial(kernel, n_s, n_t, rows, width, chunk),
            out_shape=(
                jax.ShapeDtypeStruct((rows, width), f32),
                jax.ShapeDtypeStruct((rows, width), f32),
                jax.ShapeDtypeStruct((rows, total), f32),
            ),
            in_specs=[
                pl.BlockSpec(memory_space=pltpu.HBM),
                pl.BlockSpec(memory_space=pltpu.HBM),
                pl.BlockSpec(memory_space=pltpu.HBM),
            ],
            out_specs=(pl.BlockSpec(memory_space=pltpu.VMEM),) * 3,
            scratch_shapes=[
                pltpu.SMEM((total,), jnp.int32),
                pltpu.SMEM((total,), jnp.int32),
                pltpu.VMEM((rows, width + 2 * LANE), f32),
                pltpu.VMEM((2 * LANE, 2 * LANE), f32),
                pltpu.VMEM((2, rows, LANE), jnp.int32),
                pltpu.VMEM((rows, width), f32),
                pltpu.VMEM((n_s, rows, quarter), f32),
                pltpu.VMEM((2, rows, LANE), f32),
                pltpu.VMEM((n_s, rows // 2, 2 * total), f32),
                pltpu.VMEM((n_s - 1, rows // 2, 2 * total), f32),
                pltpu.VMEM((rows // 2, 2 * total), f32),
                pltpu.VMEM((n_t, rows // 2, 2 * total), f32),
                dma((n_s,)),
                dma((2,)),
                dma((2,)),
                dma((2,)),
                dma((sends,)),
                dma((sends,)),
                dma((n_s - 1,)),
                dma((n_s - 1,)),
                dma((n_t - 1,)),
                dma((n_t - 1,)),
            ],
            compiler_params=pltpu.CompilerParams(
                collective_id=0, has_side_effects=True, vmem_limit_bytes=67043328 - 8 * rows * width - 12 * 1024 * 1024
            ),
        )(valid_start, valid_end, signal)
        return pl.pallas_call(
            flush,
            out_shape=tuple(jax.ShapeDtypeStruct(v.shape, f32) for v in kept),
            in_specs=[pl.BlockSpec(memory_space=pltpu.VMEM)] * 3,
            out_specs=(pl.BlockSpec(memory_space=pltpu.HBM),) * 3,
            scratch_shapes=[dma((2 * FLUSHES,)), dma],
            compiler_params=pltpu.CompilerParams(vmem_limit_bytes=1024 * 1024),
        )(*kept)

    in_specs = (P("series", "tm"), P(), P())
    out_specs = (P("series", "tm"), P("series", "tm"), P("series", None))
    return jax.shard_map(shards, mesh=mesh, in_specs=in_specs, out_specs=out_specs, check_vma=False)
```

```python
import functools

import jax
import jax.numpy as jnp
from jax import lax
from jax.experimental import pallas as pl
from jax.experimental.pallas import tpu as pltpu
from jax.sharding import PartitionSpec as P

HALF = 16
LANE = 128
TAPS = 2 * HALF + 1
SECOND = float(sum(j * j for j in range(-HALF, HALF + 1)))
CENTRE_SQ = SECOND / TAPS
FOURTH = float(sum((j * j - CENTRE_SQ) ** 2 for j in range(-HALF, HALF + 1)))
MESH = pl.DeviceIdType.MESH


def chunk_of(quarter):
    chunk = 1024
    while quarter % chunk:
        chunk //= 2
    return chunk


def kernel(
    n_s, n_t, rows, width, chunk,
    bounds_hbm, sig_hbm,
    smooth, slope, cov,
    bounds, ext, wts, ends, res, mixed, halo, part, r1, mine, r2,
    load_sem, bound_sem, halo_send, halo_recv, send_sem, recv_sem, s1_send, s1_recv, s2_send, s2_recv,
):
    s = lax.axis_index("series")
    t = lax.axis_index("tm")
    quarter = width // n_s
    per = quarter // chunk
    steps = n_s * per
    sends = (n_s - 1) * per
    total = n_s * rows
    tiles = chunk // LANE
    f32 = jnp.float32

    limits = pltpu.make_async_copy(bounds_hbm, bounds, bound_sem)
    limits.start()
    def offset(qi):
        if n_s == 4:
            odd = lax.rem(s, 2)
            return jnp.where(qi == 0, 2, jnp.where(qi == 1, 3 - 2 * odd, jnp.where(qi == 2, 1 + 2 * odd, 0)))
        return lax.rem(qi + 1, n_s)

    def load(qi):
        q = lax.rem(s + offset(qi), n_s)
        return pltpu.make_async_copy(
            sig_hbm.at[:, pl.ds(pl.multiple_of(q * quarter, LANE), quarter)],
            ext.at[:, pl.ds(pl.multiple_of(q * quarter + LANE, LANE), quarter)],
            load_sem.at[qi])

    for qi in range(n_s):
        load(qi).start()
    barrier = pltpu.get_barrier_semaphore()
    for d in range(1, n_s):
        pl.semaphore_signal(barrier, inc=1, device_id={"series": lax.rem(s + d, n_s)}, device_id_type=MESH)
    for d in range(1, n_t):
        pl.semaphore_signal(barrier, inc=1, device_id={"tm": lax.rem(t + d, n_t)}, device_id_type=MESH)

    tap = lax.broadcasted_iota(jnp.int32, (2 * LANE, LANE), 0) - lax.broadcasted_iota(jnp.int32, (2 * LANE, LANE), 1) - HALF
    near = (tap >= -HALF) & (tap <= HALF)
    tap = tap.astype(f32)
    wts[:, :LANE] = jnp.where(near, 1.0 / TAPS - (tap * tap - CENTRE_SQ) * (CENTRE_SQ / FOURTH), 0.0)
    wts[:, LANE:] = jnp.where(near, tap * (HALF / SECOND), 0.0)
    ext[:, :LANE] = jnp.zeros((rows, LANE), f32)
    ext[:, LANE + width :] = jnp.zeros((rows, LANE), f32)

    limits.wait()
    row = lax.broadcasted_iota(jnp.int32, (rows, LANE), 0)
    begin = t * width
    first = jnp.zeros((rows, LANE), jnp.int32)
    last = jnp.zeros((rows, LANE), jnp.int32)
    for i in range(rows):
        first = jnp.where(row == i, bounds[0, s * rows + i], first)
        last = jnp.where(row == i, bounds[1, s * rows + i], last)
    ends[0] = first - begin
    ends[1] = last - begin

    def held(v, base):
        lanes = lax.broadcasted_iota(jnp.int32, (rows, LANE), 1)
        found = []
        for spot in (ends[0] + LANE - base, ends[1] - TAPS + LANE - base):
            tile = lax.shift_right_arithmetic(spot, LANE.bit_length() - 1)
            pair = [jnp.zeros((rows, LANE), f32)] * 2
            for n in range(tiles + 1):
                here = tile == n
                for w in range(2):
                    pair[w] = jnp.where(here, v[:, (n + w) * LANE : (n + w + 1) * LANE], pair[w])
            j = lanes - (spot - tile * LANE + HALF)
            sums = []
            for j, win in ((j, pair[0]), (j + LANE, pair[1])):
                win = jnp.where((j >= -HALF) & (j <= HALF), win, 0.0)
                j = j.astype(f32)
                sums.append((win, win * j, win * (j * j - CENTRE_SQ)))
            for m, scale in enumerate((1.0 / TAPS, 1.0 / SECOND, 1.0 / FOURTH)):
                value = jnp.sum(sums[0][m] + sums[1][m], axis=1, keepdims=True) * scale
                found.append(jnp.broadcast_to(value, (rows, LANE)))
        return found

    right, left = lax.rem(t + 1, n_t), lax.rem(t + n_t - 1, n_t)
    to_right = pltpu.make_async_remote_copy(
        ext.at[:, pl.ds(width, LANE)], halo.at[0], halo_send.at[0], halo_recv.at[0],
        device_id={"tm": right}, device_id_type=MESH)
    to_left = pltpu.make_async_remote_copy(
        ext.at[:, pl.ds(LANE, LANE)], halo.at[1], halo_send.at[1], halo_recv.at[1],
        device_id={"tm": left}, device_id_type=MESH)
    def place(k):
        qi = k // per
        q = lax.rem(s + offset(qi), n_s)
        j = lax.rem(lax.rem(k, per) + 1, per)
        return q, j

    def transfer(k):
        q, j = place(k)
        return pltpu.make_async_remote_copy(
            res.at[:, pl.ds(pl.multiple_of(q * quarter + j * chunk, chunk), chunk)],
            mixed.at[s, :, pl.ds(pl.multiple_of(j * chunk, chunk), chunk)],
            send_sem.at[k], recv_sem.at[k],
            device_id={"series": q}, device_id_type=MESH)

    def spread(v):
        return jnp.concatenate([v] * tiles, axis=1)

    def step(k, carry):
        @pl.when(k == 0)
        def _():
            load(0).wait()

        @pl.when(k == 1)
        def _():
            for qi in range(1, n_s):
                load(qi).wait()

        @pl.when(k == per - 2)
        def _():
            to_right.wait_recv()
            to_left.wait_recv()
            ext[:, :LANE] = jnp.where(t == 0, 0.0, halo[0])
            ext[:, LANE + width :] = jnp.where(t == n_t - 1, 0.0, halo[1])

        q, j = place(k)
        base = pl.multiple_of(q * quarter + j * chunk, chunk)
        v = ext[:, pl.ds(base, chunk + 2 * LANE)]
        moved = pltpu.roll(v, chunk + LANE + HALF, 1)
        lines = jnp.concatenate([moved[:, n * LANE : (n + 2) * LANE] for n in range(tiles)], axis=0)
        out = jnp.dot(lines, wts[...], precision=lax.Precision.HIGHEST, preferred_element_type=f32)
        sm = jnp.concatenate([out[n * rows : (n + 1) * rows, :LANE] for n in range(tiles)], axis=1)
        sl = jnp.concatenate([out[n * rows : (n + 1) * rows, LANE:] for n in range(tiles)], axis=1)
        moment = base + lax.broadcasted_iota(jnp.int32, (rows, chunk), 1)
        low = moment - spread(ends[0])
        high = moment - spread(ends[1])
        coef = held(v, base)
        inside = (low >= 0) & (high < 0)
        below = low < HALF
        above = high >= -HALF
        along = jnp.where(below, low - HALF, high + HALF + 1).astype(f32)
        lv = jnp.where(below, spread(coef[0]), spread(coef[3]))
        tl = jnp.where(below, spread(coef[1]), spread(coef[4]))
        bd = jnp.where(below, spread(coef[2]), spread(coef[5]))
        end = below | above
        sm = jnp.where(end, lv + tl * along + bd * (along * along - CENTRE_SQ), sm)
        sl = jnp.where(end, HALF * (tl + 2.0 * along * bd), sl)
        sm = jnp.where(inside, sm, 0.0)
        smooth[:, pl.ds(base, chunk)] = sm
        slope[:, pl.ds(base, chunk)] = jnp.where(inside, sl, 0.0)
        rs = jnp.where(inside, v[:, LANE : LANE + chunk] - sm, 0.0)

        @pl.when(k < sends)
        def _():
            res[:, pl.ds(base, chunk)] = rs

        @pl.when(k >= sends)
        def _():
            mixed[s, :, pl.ds(pl.multiple_of(j * chunk, chunk), chunk)] = rs

        @pl.when(k == 0)
        def _():
            pl.semaphore_wait(barrier, n_s - 1 + n_t - 1)

        @pl.when(k == 1)
        def _():
            to_right.start()
            to_left.start()

        @pl.when((k >= 1) & (k <= sends))
        def _():
            transfer(k - 1).start()

        return carry

    lax.fori_loop(0, steps, step, 0)

    def arrival(k, i):
        src = lax.rem(s + n_s - offset(k // per), n_s)
        j = (i + 1) % per
        return pltpu.make_async_remote_copy(
            res.at[:, pl.ds(0, chunk)],
            mixed.at[src, :, pl.ds(pl.multiple_of(j * chunk, chunk), chunk)],
            send_sem.at[k], recv_sem.at[k],
            device_id={"series": src}, device_id_type=MESH)

    half = rows // 2
    left_half = lax.broadcasted_iota(jnp.int32, (half, 2 * total), 1) < total

    def pack(v):
        return jnp.where(left_half, v[:half], v[half:])

    gram = jnp.zeros((2 * total, 2 * total), f32)
    for i in range(per):
        for qi in range(n_s - 1):
            arrival(qi * per + i, i).wait_recv()
        j = (i + 1) % per
        x = jnp.concatenate(
            [mixed[g, :, pl.ds(pl.multiple_of(j * chunk, chunk), chunk)] for g in range(n_s)], axis=0)
        hi = x.astype(jnp.bfloat16)
        lo = (x - hi.astype(f32)).astype(jnp.bfloat16)
        z = jnp.concatenate([hi, lo], axis=0)
        gram = gram + lax.dot_general(z, z, (((1,), (1,)), ((), ())), preferred_element_type=f32)
    both = gram[:total] + gram[total:]
    both = both + pltpu.roll(both, total, 1)
    for g in range(n_s):
        part[g] = pack(both[g * rows : (g + 1) * rows])

    def first_stage(d):
        peer = lax.rem(s + d, n_s)
        return pltpu.make_async_remote_copy(
            part.at[peer], r1.at[d - 1], s1_send.at[d - 1], s1_recv.at[d - 1],
            device_id={"series": peer}, device_id_type=MESH)

    for d in range(1, n_s):
        first_stage(d).start()

    lane = lax.broadcasted_iota(jnp.int32, (rows, 2 * total), 1)
    lane = jnp.where(lane < total, lane, lane - total)
    first_k = jnp.zeros((rows, 2 * total), jnp.int32)
    last_k = jnp.zeros((rows, 2 * total), jnp.int32)
    for i in range(total):
        first_k = jnp.where(lane == i, bounds[0, i], first_k)
        last_k = jnp.where(lane == i, bounds[1, i], last_k)
    count = pack((jnp.minimum(last_k, last) - jnp.maximum(first_k, first)).astype(f32))

    own = part[s]
    for d in range(1, n_s):
        first_stage(d).wait_recv()
        own = own + r1[d - 1]
    mine[...] = own

    def second_stage(d):
        return pltpu.make_async_remote_copy(
            mine, r2.at[t], s2_send.at[d - 1], s2_recv.at[d - 1],
            device_id={"tm": lax.rem(t + d, n_t)}, device_id_type=MESH)

    def second_arrival(d):
        src = lax.rem(t + n_t - d, n_t)
        return pltpu.make_async_remote_copy(
            mine, r2.at[src], s2_send.at[d - 1], s2_recv.at[d - 1],
            device_id={"tm": src}, device_id_type=MESH)

    for d in range(1, n_t):
        second_stage(d).start()
    r2[t] = own
    for k in range(sends):
        transfer(k).wait_send()
    to_right.wait_send()
    to_left.wait_send()
    for d in range(1, n_s):
        first_stage(d).wait_send()
    for d in range(1, n_t):
        second_arrival(d).wait_recv()
    full = r2[0]
    for d in range(1, n_t):
        full = full + r2[d]
    full = full / count
    cov[:half] = full[:, :total]
    cov[half:] = pltpu.roll(full, total, 1)[:, :total]
    for d in range(1, n_t):
        second_stage(d).wait_send()


FLUSHES = 4


def flush(smooth, slope, cov, smooth_out, slope_out, cov_out, sems, cov_sem):
    piece = smooth.shape[1] // FLUSHES
    copies = [pltpu.make_async_copy(cov, cov_out, cov_sem)]
    for i in range(FLUSHES):
        span = pl.ds(i * piece, piece)
        copies.append(pltpu.make_async_copy(smooth.at[:, span], smooth_out.at[:, span], sems.at[2 * i]))
        copies.append(pltpu.make_async_copy(slope.at[:, span], slope_out.at[:, span], sems.at[2 * i + 1]))
    for copy in copies:
        copy.start()
    for copy in copies:
        copy.wait()


def solution(mesh):
    n_t, n_s = mesh.shape["tm"], mesh.shape["series"]

    def shards(signal, valid_start, valid_end):
        rows, width = signal.shape
        total = rows * n_s
        quarter = width // n_s
        chunk = chunk_of(quarter)
        sends = (n_s - 1) * (quarter // chunk)
        f32 = jnp.float32
        dma = pltpu.SemaphoreType.DMA
        kept = pl.pallas_call(
            functools.partial(kernel, n_s, n_t, rows, width, chunk),
            out_shape=(
                jax.ShapeDtypeStruct((rows, width), f32),
                jax.ShapeDtypeStruct((rows, width), f32),
                jax.ShapeDtypeStruct((rows, total), f32),
            ),
            in_specs=[
                pl.BlockSpec(memory_space=pltpu.HBM),
                pl.BlockSpec(memory_space=pltpu.HBM),
            ],
            out_specs=(pl.BlockSpec(memory_space=pltpu.VMEM),) * 3,
            scratch_shapes=[
                pltpu.SMEM((2, total), jnp.int32),
                pltpu.VMEM((rows, width + 2 * LANE), f32),
                pltpu.VMEM((2 * LANE, 2 * LANE), f32),
                pltpu.VMEM((2, rows, LANE), jnp.int32),
                pltpu.VMEM((rows, width), f32),
                pltpu.VMEM((n_s, rows, quarter), f32),
                pltpu.VMEM((2, rows, LANE), f32),
                pltpu.VMEM((n_s, rows // 2, 2 * total), f32),
                pltpu.VMEM((n_s - 1, rows // 2, 2 * total), f32),
                pltpu.VMEM((rows // 2, 2 * total), f32),
                pltpu.VMEM((n_t, rows // 2, 2 * total), f32),
                dma((n_s,)),
                dma,
                dma((2,)),
                dma((2,)),
                dma((sends,)),
                dma((sends,)),
                dma((n_s - 1,)),
                dma((n_s - 1,)),
                dma((n_t - 1,)),
                dma((n_t - 1,)),
            ],
            compiler_params=pltpu.CompilerParams(
                collective_id=0, has_side_effects=True, vmem_limit_bytes=67043328 - 8 * rows * width - 12 * 1024 * 1024
            ),
        )(jnp.stack([valid_start, valid_end]), signal)
        return pl.pallas_call(
            flush,
            out_shape=tuple(jax.ShapeDtypeStruct(v.shape, f32) for v in kept),
            in_specs=[pl.BlockSpec(memory_space=pltpu.VMEM)] * 3,
            out_specs=(pl.BlockSpec(memory_space=pltpu.HBM),) * 3,
            scratch_shapes=[dma((2 * FLUSHES,)), dma],
            compiler_params=pltpu.CompilerParams(vmem_limit_bytes=1024 * 1024),
        )(*kept)

    in_specs = (P("series", "tm"), P(), P())
    out_specs = (P("series", "tm"), P("series", "tm"), P("series", None))
    return jax.shard_map(shards, mesh=mesh, in_specs=in_specs, out_specs=out_specs, check_vma=False)
```
